32 devices in a mesh: seq: 8 (over z, x), mp: 4 (over y, core).
Axes of the slice: x: 2, y: 2, z: 4, core: 2. Of those that a mesh axis runs over, the one named last changes fastest.
Arguments:
- tokens: bfloat16 [256, 3584], P('mp'), may hold values from -6 to 6
- gain_attn: float32 [3584], replicated, may hold values from 0.25 to 1.75
- w_query: bfloat16 [3584, 3584], P(None, 'seq'), may hold values from -0.09375 to 0.09375
- query_bias: float32 [3584], P('seq'), may hold values from -3 to 3
- cache_keys: bfloat16 [4, 8192, 128], P(None, 'seq'), may hold values from -80 to 80
- cache_values: bfloat16 [4, 8192, 128], P(None, 'seq'), may hold values from -6 to 6
- w_out: bfloat16 [3584, 3584], P(None, 'seq'), may hold values from -0.09375 to 0.09375
- gain_ffn: float32 [3584], P('seq'), may hold values from 0.25 to 1.75
- w_gate: bfloat16 [3584, 18944], P('mp', 'seq'), may hold values from -0.09375 to 0.09375
- w_up: bfloat16 [3584, 18944], P('mp', 'seq'), may hold values from -0.09375 to 0.09375
- w_down: bfloat16 [18944, 3584], P('seq', 'mp'), may hold values from -0.0625 to 0.0625
Outputs:
- attended: bfloat16 [256, 3584], P('mp', 'seq')
- layer_out: bfloat16 [256, 3584], P('mp', 'seq')
The draws below stay inside these ranges and needn't reach their ends.
All inputs are finite; a program needn't handle non-finite values.
Results may differ from the reference program's by a relative error of at most 0.012.
The reference program's roundings to bfloat16 on the way (of `normed`, `queries`, `normed_ffn` and `activated`) count: a program that leaves them out, or rounds other values in their place, can miss the bound.
Values may be sent and summed in bfloat16 or wider, within the bound.
A program may use at most 64 MiB of HBM per device.

```python
import jax
import jax.numpy as jnp
from jax import lax

D = 3584
HEADS = 28
KV_HEADS = 4
HEAD = 128
FF = 18944
CTX_DEV = 1024
QUERIES = 256
CONTEXT = 8192
N_SEQ = 8


def draw_cache_keys(key, part):
    shape = (KV_HEADS, CONTEXT, HEAD)
    base_key, heavy_key, pick_key = jax.random.split(jax.random.fold_in(key, 17), 3)
    drawn = jnp.clip(2.7 * jax.random.normal(base_key, shape, jnp.float32), -16.0, 16.0)
    return drawn.astype(jnp.bfloat16)


def raised(values, own_key, source, target, blocks, factor):
    def block_of(axis_at):
        return (jnp.arange(values.shape[axis_at]) // (values.shape[axis_at] // blocks)).reshape((-1,) + (1,) * (values.ndim - 1 - axis_at))

    first = jax.random.permutation(own_key, blocks)[block_of(target)]
    far = (block_of(target) + blocks // 2) % blocks
    return jnp.where((block_of(source) == first) | (block_of(source) == far), factor * values, values)


def shard_levels(rng, extent, cuts, least, largest):
    loudness = 1.0
    for axis_at, blocks in cuts:
        draws = jax.random.uniform(jax.random.fold_in(jax.random.fold_in(rng, 6), axis_at), (blocks,), jnp.float32, least / len(cuts), largest / len(cuts))
        loudness = loudness * jnp.repeat(jnp.exp(draws), extent[axis_at] // blocks).reshape((-1,) + (1,) * (len(extent) - 1 - axis_at))
    return loudness


def centred(stream_key, extent, width, most, cuts=(), held_as=jnp.bfloat16):
    loudness = shard_levels(stream_key, extent, cuts, -0.22, 0.18) if cuts else 1.0
    values = jax.random.normal(stream_key, extent, jnp.float32) * width * loudness
    return jnp.minimum(jnp.maximum(values, -most), most).astype(held_as)


def heavy_noise(rng, dims, spread, most, cuts, heavy, kind=jnp.bfloat16):
    entries = spread * jax.random.normal(rng, dims, jnp.float32)
    if cuts:
        entries = entries * shard_levels(rng, dims, cuts, -0.22, 0.18)
    return jnp.clip(raised(entries, jax.random.fold_in(rng, 3), *heavy), -most, most).astype(kind)


def setup_inputs(seed: int = 0) -> dict:
    keys = jax.random.split(jax.random.key(seed), 12)
    return {
        "tokens": centred(keys[0], (QUERIES, D), 1.0, 6.0, ((0, 4),)),
        "gain_attn": jnp.clip(1.0 + 0.15 * jax.random.normal(keys[1], (D,), jnp.float32), 0.25, 1.75),
        "w_query": centred(keys[2], (D, D), D ** -0.5, 0.09375, ((1, 8),)),
        "query_bias": centred(keys[3], (D,), 0.5, 3.0, ((0, 8),), jnp.float32),
        "cache_keys": draw_cache_keys(jax.random.fold_in(keys[11], 71), 0),
        "cache_values": centred(keys[5], (KV_HEADS, CONTEXT, HEAD), 1.0, 6.0, ((1, 8),)),
        "w_out": centred(keys[6], (D, D), D ** -0.5, 0.09375, ((1, 8),)),
        "gain_ffn": jnp.clip(1.0 + 0.15 * jax.random.normal(keys[7], (D,), jnp.float32), 0.25, 1.75),
        "w_gate": centred(keys[8], (D, FF), D ** -0.5, 0.09375, ((0, 4), (1, 8))),
        "w_up": centred(keys[9], (D, FF), D ** -0.5, 0.09375, ((0, 4), (1, 8))),
        "w_down": heavy_noise(keys[10], (FF, D), FF ** -0.5, 0.0625, ((0, 8), (1, 4)), (0, 1, 8, 2.0)),
    }


eps = 1e-06

def expand(per_head):
    return jnp.repeat(per_head, HEAD, axis=1)

def block_attention(queries, block_keys, block_values):
    row_count = queries.shape[0]
    group_size = HEADS // KV_HEADS
    shaped = queries.reshape(row_count, KV_HEADS, group_size * HEAD)
    maxima = []
    sums = []
    outputs = []
    for head_group in range(KV_HEADS):
        block_query = shaped[:, head_group, :].reshape(row_count * group_size, HEAD)
        scores = jnp.einsum('rd,kd->rk', block_query.astype(jnp.float32), block_keys[head_group].astype(jnp.float32)) * HEAD ** (-0.5)
        highest = lax.optimization_barrier(jnp.max(scores, axis=1, keepdims=True))
        probs = jnp.exp(scores - highest)
        weight_sum = lax.optimization_barrier(jnp.sum(probs, axis=1))
        weighted = jnp.dot(probs.astype(jnp.bfloat16), block_values[head_group], preferred_element_type=jnp.float32)
        maxima.append(highest.reshape(row_count, group_size))
        sums.append(weight_sum.reshape(row_count, group_size))
        outputs.append(weighted.reshape(row_count, group_size * HEAD))
    return (jnp.concatenate(maxima, axis=1), jnp.concatenate(sums, axis=1), jnp.concatenate(outputs, axis=1))

def combine(first, second):
    highest = jnp.maximum(first[0], second[0])
    scale_one = jnp.exp(first[0] - highest)
    scale_two = jnp.exp(second[0] - highest)
    weight_sum = first[1] * scale_one + second[1] * scale_two
    weighted = first[2] * expand(scale_one) + second[2] * expand(scale_two)
    return (highest, weight_sum, weighted)

def reference(tokens, gain_attn, w_query, query_bias, cache_keys, cache_values, w_out, gain_ffn, w_gate, w_up, w_down):
    hidden_in = tokens.astype(jnp.float32)
    mean_sq = lax.optimization_barrier(jnp.mean(hidden_in * hidden_in, axis=1, keepdims=True))
    normed = (hidden_in * lax.rsqrt(mean_sq + eps) * gain_attn).astype(jnp.bfloat16)
    queries = (jnp.dot(normed, w_query, preferred_element_type=jnp.float32) + query_bias).astype(jnp.bfloat16)
    key_blocks = cache_keys.reshape(KV_HEADS, N_SEQ, CTX_DEV, HEAD).transpose(1, 0, 2, 3)
    value_blocks = cache_values.reshape(KV_HEADS, N_SEQ, CTX_DEV, HEAD).transpose(1, 0, 2, 3)
    start_state = block_attention(queries, key_blocks[0], value_blocks[0])

    def absorb(carried, blocks):
        return (combine(carried, block_attention(queries, blocks[0], blocks[1])), None)
    final_state, unused = lax.scan(absorb, start_state, (key_blocks[1:], value_blocks[1:]))
    attended = (final_state[2] / expand(final_state[1])).astype(jnp.bfloat16)
    residual = hidden_in + jnp.dot(attended, w_out, preferred_element_type=jnp.float32)
    mean_res = lax.optimization_barrier(jnp.mean(residual * residual, axis=1, keepdims=True))
    normed_ffn = (residual * lax.rsqrt(mean_res + eps) * gain_ffn).astype(jnp.bfloat16)
    gate_proj = jnp.dot(normed_ffn, w_gate, preferred_element_type=jnp.float32)
    up_proj = jnp.dot(normed_ffn, w_up, preferred_element_type=jnp.float32)
    activated = (jax.nn.silu(gate_proj) * up_proj).astype(jnp.bfloat16)
    ffn_sum = jnp.dot(activated, w_down, preferred_element_type=jnp.float32)
    layer_out = (residual + ffn_sum).astype(jnp.bfloat16)
    return (attended, layer_out)
```

```python
import functools
import math
import types

import jax
import jax.numpy as jnp
from jax import lax
from jax.experimental import pallas as pl
from jax.experimental.pallas import tpu as pltpu
from jax.sharding import PartitionSpec as P

D = 3584
HEADS = 28
KV_HEADS = 4
HEAD = 128
GROUP = HEADS // KV_HEADS
SUM_ROW = 8
CHUNKS = 2
HALVES = 2

eps = 1e-06
EXP2_SCALE = HEAD ** (-0.5) * math.log2(math.e)
MESH = pl.DeviceIdType.MESH
VMEM = pltpu.VMEM
ARGS = (
    "tokens_hbm", "gain_attn_hbm", "w_query_hbm", "bias_hbm", "keys_hbm", "values_hbm",
    "w_out_hbm", "gain_ffn_hbm", "gate_hbm", "up_hbm", "down_hbm",
)
OUTS = ("attended", "out")


def push(src, dst, send, recv, to):
    return pltpu.make_async_remote_copy(
        src_ref=src,
        dst_ref=dst,
        send_sem=send,
        recv_sem=recv,
        device_id=to,
        device_id_type=MESH,
    )


def times_transposed(a, b):
    return lax.dot_general(a, b, (((1,), (1,)), ((), ())), preferred_element_type=jnp.float32)


def row_to_column(row):
    k = row.shape[1]
    across = lax.broadcasted_iota(jnp.int32, (k, k), 1)
    down = lax.broadcasted_iota(jnp.int32, (k, k), 0)
    return jnp.sum(jnp.where(across == down, row, 0.0), axis=1, keepdims=True)


def column_to_row(column):
    k = column.shape[0]
    across = lax.broadcasted_iota(jnp.int32, (k, k), 1)
    down = lax.broadcasted_iota(jnp.int32, (k, k), 0)
    return jnp.sum(jnp.where(across == down, column, 0.0), axis=0, keepdims=True)


class Place:
    def __init__(self, n, n_mp):
        self.n, self.n_mp = n, n_mp
        self.lines, self.per, self.wide = n // 2, n // n_mp, n // KV_HEADS
        self.s, self.m = lax.axis_index("seq"), lax.axis_index("mp")
        self.hi, self.lo = self.s // 2, lax.rem(self.s, 2)
        self.y, self.core = self.m // 2, lax.rem(self.m, 2)
        self.partner = (self.hi * 2 + 1 - self.lo, self.m)
        self.sibling = (self.s, self.y * 2 + (1 - self.core))
        self.across = (self.s, (1 - self.y) * 2 + self.core)

    def ahead(self, d):
        return lax.rem(self.hi + d, self.lines)

    def behind(self, d):
        return lax.rem(self.hi + self.lines - d, self.lines)

    def near(self, b, m):
        return (self.hi * 2 + lax.rem(self.lo + b, 2), m)

    def group(self, j):
        return lax.rem(self.s // self.wide + KV_HEADS - j, KV_HEADS)


def greet(at):
    barrier = pltpu.get_barrier_semaphore()
    peers = [(lax.rem(at.s + d, at.n), at.m) for d in range(1, at.n)]
    peers += [
        at.near(b, lax.rem(at.m + i, at.n_mp)) for i in range(1, at.n_mp) for b in range(2)
    ]
    for peer in peers:
        pl.semaphore_signal(barrier, inc=1, device_id=peer, device_id_type=MESH)
    return lambda: pl.semaphore_wait(barrier, len(peers))


class Gather:
    def __init__(self, at, buf, sems):
        self.at, self.buf, self.sems = at, buf, sems
        self.direct = [
            push(
                buf.at[at.s], buf.at[at.s], sems.at[0, d], sems.at[1, d],
                (at.ahead(d) * 2 + at.lo, at.m),
            )
            for d in range(1, at.lines)
        ]
        self.handed, self.taken = [], 0

    def start(self):
        for copy in self.direct:
            copy.start()
        self.hand(0)

    def hand(self, d):
        at = self.at
        if d < len(self.handed):
            return
        if d:
            self.direct[d - 1].wait_recv()
        block = self.buf.at[at.behind(d) * 2 + at.lo]
        copy = push(block, block, self.sems.at[2, d], self.sems.at[3, d], at.partner)
        copy.start()
        self.handed.append(copy)

    def take(self, j):
        last = j if self.at.lines == KV_HEADS else self.at.lines - 1
        while self.taken <= last:
            self.hand(self.taken)
            self.handed[self.taken].wait_recv()
            self.taken += 1

    def left(self):
        for copy in self.direct + self.handed:
            copy.wait_send()


def layer_kernel(n, n_mp, bounds, names, *refs):
    R = types.SimpleNamespace(**dict(zip(names, refs)))
    at = Place(n, n_mp)
    s, m, hi, lo, y, core = at.s, at.m, at.hi, at.lo, at.y, at.core
    per, wide, lines = at.per, at.wide, at.lines
    rows, width = R.out.shape[0] // HALVES, R.out.shape[1]
    bf16, f32 = jnp.bfloat16, jnp.float32
    sends = []

    def part(h):
        return slice(h * rows, (h + 1) * rows)

    loads = {}
    slots = iter(range(R.w_sems.shape[0]))

    def load(name, src, dst):
        loads[name] = pltpu.make_async_copy(src, dst, R.w_sems.at[next(slots)])
        loads[name].start()

    load("tokens", R.tokens_hbm, R.tokens)
    load("gain_attn", R.gain_attn_hbm, R.gain_attn)
    load("bias", R.bias_hbm, R.bias)
    load("w_query", R.w_query_hbm, R.w_query)
    load("keys", R.keys_hbm, R.keys)
    load("values", R.values_hbm, R.values)
    load("gain_ffn", R.gain_ffn_hbm, R.gain_ffn)
    span = D // KV_HEADS
    for g in range(KV_HEADS):
        load(f"w_out{g}", R.w_out_hbm.at[:, pl.ds(g * span, span)], R.w_out.at[g])
    load("gate", R.gate_hbm, R.gate_w)
    load("up", R.up_hbm, R.up_w)
    load("down", R.down_hbm, R.down_w)
    everyone_here = greet(at)

    loads["tokens"].wait()
    hidden_in = R.tokens[...].astype(f32)
    mean_sq = jnp.sum(hidden_in * hidden_in, axis=1, keepdims=True) / D
    loads["gain_attn"].wait()
    normed = (hidden_in * lax.rsqrt(mean_sq + eps) * R.gain_attn[...]).astype(bf16)
    loads["bias"].wait()
    loads["w_query"].wait()
    queries = (times_transposed(normed, R.w_query[...]) + R.bias[...]).astype(bf16)
    for h in range(HALVES):
        R.qbuf[h, s] = queries[part(h)]
    everyone_here()
    asked = [Gather(at, R.qbuf.at[h], R.q_sems.at[h]) for h in range(HALVES)]
    for flow in asked:
        flow.start()
    for k in range(n):

        @pl.when(s == k)
        def _():
            R.own_tokens[...] = R.tokens[:, k * width : (k + 1) * width].astype(f32)

    def attend(h, j):
        g = at.group(j)
        q = jnp.concatenate([R.qbuf[h, g * wide + i] for i in range(wide)], axis=1)
        stacked = jnp.concatenate([q[:, i * HEAD : (i + 1) * HEAD] for i in range(GROUP)], axis=0)
        scores = times_transposed(stacked, R.keys[g])
        highest = jnp.max(scores, axis=1, keepdims=True)
        probs = jnp.exp2((scores - highest) * EXP2_SCALE)
        sums = jnp.sum(probs, axis=1, keepdims=True)
        weighted = jnp.dot(probs.astype(bf16), R.values[g], preferred_element_type=f32)
        side = jnp.concatenate([weighted[part(i)] for i in range(GROUP)], axis=1).astype(bf16)
        for i in range(wide):
            R.part_out[h, g * wide + i] = side[:, i * width : (i + 1) * width]
        R.stat_out[h, g] = jnp.zeros((2 * SUM_ROW, rows), f32)
        for i in range(GROUP):
            R.stat_out[h, g, i : i + 1, :] = column_to_row(highest[part(i)] * EXP2_SCALE)
            R.stat_out[h, g, i + SUM_ROW : i + SUM_ROW + 1, :] = column_to_row(sums[part(i)])
        for i in range(wide):
            to = g * wide + lax.rem(s + i, wide)
            if i == 0 and j == 0:
                R.part_in[h, s] = R.part_out[h, s]
                R.stat_in[h, s] = R.stat_out[h, g]
                continue
            for src, dst, k in (
                (R.part_out.at[h, to], R.part_in.at[h, s], 0),
                (R.stat_out.at[h, g], R.stat_in.at[h, s], 1),
            ):
                copy = push(
                    src, dst, R.m_send.at[h, k, j * wide + i], R.m_recv.at[h, k, s], (to, m)
                )
                copy.start()
                sends.append(copy)

    def merge(h):
        for d in range(1, n):
            source = lax.rem(s + d, n)
            for src, dst, k in (
                (R.part_out.at[h, 0], R.part_in.at[h, source], 0),
                (R.stat_out.at[h, 0], R.stat_in.at[h, source], 1),
            ):
                sem = R.m_recv.at[h, k, source]
                push(src, dst, sem, sem, (source, m)).wait_recv()
        maxima, sums = R.stat_in[h, :, :SUM_ROW, :], R.stat_in[h, :, SUM_ROW:, :]
        rescale = jnp.exp2(maxima - jnp.max(maxima, axis=0, keepdims=True))
        total = jnp.sum(sums * rescale, axis=0)
        row = lax.broadcasted_iota(jnp.int32, (SUM_ROW, rows), 0)
        inverse = 1.0 / jnp.where(row < GROUP, total, 1.0)
        shape = (2 * SUM_ROW, width)
        column = s * width + lax.broadcasted_iota(jnp.int32, shape, 1)
        head = lax.div(column, HEAD) - s // wide * GROUP
        index = lax.rem(lax.broadcasted_iota(jnp.int32, shape, 0), SUM_ROW)
        pick = jnp.where(head == index, 1.0, 0.0).astype(bf16)
        result = jnp.zeros((rows, width), f32)
        for j in range(n):
            exact = rescale[j] * inverse
            coarse = exact.astype(bf16).astype(f32)
            pair = jnp.concatenate([coarse, exact - coarse], axis=0).astype(bf16)
            factor = lax.dot_general(
                pair, pick, (((0,), (0,)), ((), ())), preferred_element_type=f32
            )
            result = result + R.part_in[h, j].astype(f32) * factor
        R.att[h, s] = result.astype(bf16)
        R.attended[part(h), :] = result.astype(bf16)

    def project(h, flow):
        total = R.own_tokens[part(h), :]
        for j in range(KV_HEADS):
            flow.take(j)
            g = at.group(j)
            block = jnp.concatenate([R.att[h, g * wide + i] for i in range(wide)], axis=1)
            total = total + times_transposed(block, R.w_out[g])
        R.residual[part(h), :] = total
        R.lined[h, hi] = (total * R.gain_ffn[...]).astype(bf16)
        R.squares[h, s] = column_to_row(jnp.sum(total * total, axis=1, keepdims=True))
        for d in range(1, lines):
            copy = push(
                R.lined.at[h, hi], R.lined.at[h, hi], R.l_sems.at[h, 0, d], R.l_sems.at[h, 1, d],
                (at.ahead(d) * 2 + lo, m),
            )
            copy.start()
            lined[h].append(copy)
        for d in range(1, n):
            copy = push(
                R.squares.at[h, s], R.squares.at[h, s], R.sq_sems.at[h, 0, d],
                R.sq_sems.at[h, 1, d], (lax.rem(s + d, n), m),
            )
            copy.start()
            squared[h].append(copy)

    lined = [[] for _ in range(HALVES)]
    squared = [[] for _ in range(HALVES)]
    relayed = []

    def relay(h):
        for d in range(lines):
            if d:
                lined[h][d - 1].wait_recv()
            line = at.behind(d)
            source = line * 2 + lo
            to_m, k = source // per, lax.rem(source, per)
            for b in range(2):
                copy = push(
                    R.lined.at[h, line], R.blocks.at[h, m, k], R.r_send.at[h, b, d],
                    R.r_recv.at[h, m, k], at.near(b, to_m),
                )
                if b:
                    copy.start()
                    sends.append(copy)
                    continue
                here = to_m == m

                @pl.when(here)
                def _():
                    R.blocks[h, m, k] = R.lined[h, line]

                @pl.when(jnp.logical_not(here))
                def _():
                    copy.start()

                relayed.append((here, copy))

    order = (1 - core, 3 - core, core, 2 + core)

    def collect(h):
        for i in range(n_mp):
            source = lax.rem(m + i, n_mp)
            for k in range(per):
                if i == 0 and k % 2 == 0:
                    continue
                at_k = k // 2 * 2 + lax.rem(lo + k, 2)
                sem = R.r_recv.at[h, source, at_k]
                push(
                    R.lined.at[h, 0], R.blocks.at[h, source, at_k], sem, sem,
                    at.near(k % 2, source),
                ).wait_recv()
        for p, t in enumerate(order):
            R.features[h, p * rows : (p + 1) * rows, :] = jnp.concatenate(
                [R.blocks[h, t, j] for j in range(per)], axis=1
            )

    def inverse_of(h):
        for copy in squared[h]:
            copy.wait_recv()
        return row_to_column(lax.rsqrt(jnp.sum(R.squares[h], axis=0) / D + eps))

    chunks = []
    for c, (h, first, last) in enumerate(bounds):
        kept, s1_out, s1_in, s2_out, s2_in, act = (
            getattr(R, f"{name}{c}") for name in ("kept", "s1_out", "s1_in", "s2_out", "s2_in", "act")
        )
        sem = lambda k, c=c: R.c_sems.at[c, k]
        chunks.append(
            dict(
                half=h, first=first, last=last, kept=kept, s1_out=s1_out, s1_in=s1_in,
                s2_out=s2_out, s2_in=s2_in, act=act,
                s1=push(s1_out, s1_in, sem(0), sem(1), at.sibling),
                s2=push(s2_out, s2_in, sem(2), sem(3), at.across),
                near=push(act.at[m], act.at[m], sem(4), sem(5), at.sibling),
                far=push(act.at[m], act.at[m], sem(6), sem(7), at.across),
                relay=push(
                    act.at[at.across[1]], act.at[at.across[1]], sem(8), sem(9), at.sibling
                ),
            )
        )
    halves = [[ch for ch in chunks if ch["half"] == h] for h in range(HALVES)]

    def multiply(ch):
        for g, weight in enumerate((R.gate_w, R.up_w)):
            product = times_transposed(R.features[ch["half"]], weight[ch["first"] : ch["last"], :])
            for p in range(2):
                ch["s1_out"][g, p] = product[p * rows : (p + 1) * rows].astype(bf16)
                ch["kept"][g, p] = product[(p + 2) * rows : (p + 3) * rows]
        ch["s1"].start()

    def pair_sum(ch):
        ch["s1"].wait_recv()
        for g in range(2):
            ch["s2_out"][g] = (
                ch["kept"][g, 1 - y] + ch["s1_in"][g, 1 - y].astype(f32)
            ).astype(bf16)
        ch["s2"].start()

    def activate(ch, inverse):
        ch["s2"].wait_recv()
        gate, up = [
            (ch["kept"][g, y] + ch["s1_in"][g, y].astype(f32) + ch["s2_in"][g].astype(f32))
            * inverse
            for g in range(2)
        ]
        ch["act"][m] = (gate / (1.0 + jnp.exp(-gate)) * up).astype(bf16)
        ch["far"].start()
        ch["near"].start()

    def finish(h):
        own = halves[h]
        for c, ch in enumerate(own):
            ch["far"].wait_recv()
            ch["relay"].start()
            ch["near"].wait_recv()
            ch["relay"].wait_recv()
            act = ch["act"][...].reshape(n_mp * rows, ch["last"] - ch["first"])
            product = jnp.dot(
                act, R.down_w[ch["first"] : ch["last"], :], preferred_element_type=f32
            )
            total = product if c == 0 else R.acc[...] + product
            if c < len(own) - 1:
                R.acc[...] = total
        for t in range(n_mp):
            for k in range(per):
                R.down_out[h, t, k % 2, k // 2] = total[
                    t * rows : (t + 1) * rows, k * width : (k + 1) * width
                ].astype(bf16)
        for i in range(n_mp):
            for b in range(2):
                if i == 0 and b == 0:
                    R.home_in[h, lo, m] = R.down_out[h, m, lo]
                    continue
                to_m, to_lo = lax.rem(m + i, n_mp), lax.rem(lo + b, 2)
                copy = push(
                    R.down_out.at[h, to_m, to_lo], R.home_in.at[h, lo, m],
                    R.h_sems.at[h, 0, i * 2 + b], R.h_sems.at[h, 1, i * 2 + b], at.near(b, to_m),
                )
                copy.start()
                homed[h].append(copy)

    homed = [[] for _ in range(HALVES)]
    lastly = []

    def send_home(h):
        arrivals = iter(homed[h])
        for i in range(n_mp):
            source = lax.rem(m + n_mp - i, n_mp)
            for b in range(2):
                if i or b:
                    next(arrivals).wait_recv()
            for k in range(per // 2):
                line = source * (per // 2) + k
                total = R.home_in[h, 0, source, k].astype(f32) + R.home_in[h, 1, source, k].astype(f32)
                R.home_out[h, line] = total.astype(bf16)
                here = line == hi
                copy = push(
                    R.home_out.at[h, line], R.terms.at[h, hi], R.t_send.at[h, line],
                    R.t_recv.at[h, hi], (line * 2 + lo, m),
                )

                @pl.when(here)
                def _():
                    R.terms[h, hi] = R.home_out[h, line]

                @pl.when(jnp.logical_not(here))
                def _():
                    copy.start()

                lastly.append((here, copy))

    def conclude(h):
        for d in range(1, lines):
            line = at.behind(d)
            sem = R.t_recv.at[h, line]
            push(
                R.home_out.at[h, 0], R.terms.at[h, line], sem, sem, (line * 2 + lo, m)
            ).wait_recv()
        result = R.residual[part(h), :]
        for i in range(lines):
            result = result + R.terms[h, i].astype(f32)
        R.out[part(h), :] = result.astype(bf16)

    loads["keys"].wait()
    loads["values"].wait()
    for h in range(HALVES):
        for j in range(KV_HEADS):
            asked[h].take(j)
            if h + 1 < HALVES and lines == KV_HEADS:
                asked[h + 1].hand(j)
            attend(h, j)
    for g in range(KV_HEADS):
        loads[f"w_out{g}"].wait()
    loads["gain_ffn"].wait()
    answered = [Gather(at, R.att.at[h], R.a_sems.at[h]) for h in range(HALVES)]
    for h in range(HALVES):
        merge(h)
        answered[h].start()
    for h in range(HALVES):
        project(h, answered[h])
    relay(0)
    collect_next = 0
    loads["gate"].wait()
    loads["up"].wait()
    for h in range(1, HALVES):
        relay(h)
    collect(0)
    for c, ch in enumerate(halves[0]):
        multiply(ch)
        if c >= 1:
            pair_sum(halves[0][c - 1])
    pair_sum(halves[0][-1])
    inverse = [None] * HALVES
    inverse[0] = inverse_of(0)
    for h in range(1, HALVES):
        collect(h)
        for ch in halves[h]:
            multiply(ch)
        for ch in halves[h - 1]:
            activate(ch, inverse[h - 1])
        for ch in halves[h]:
            pair_sum(ch)
        inverse[h] = inverse_of(h)
        if h == 1:
            loads["down"].wait()
        else:
            send_home(h - 2)
        finish(h - 1)
    for ch in halves[-1]:
        activate(ch, inverse[-1])
    send_home(HALVES - 2)
    finish(HALVES - 1)
    send_home(HALVES - 1)
    for h in range(HALVES):
        conclude(h)

    for flow in asked + answered:
        flow.left()
    for copies in lined + squared + homed:
        sends.extend(copies)
    for copy in sends:
        copy.wait_send()
    for here, copy in relayed + lastly:

        @pl.when(jnp.logical_not(here))
        def _():
            copy.wait_send()

    for ch in chunks:
        for name in ("s1", "s2", "near", "far", "relay"):
            ch[name].wait_send()


def layer(n, n_mp, *arrays):
    tokens, w_query, keys, w_gate, w_down = (arrays[i] for i in (0, 2, 4, 8, 10))
    rows, width = tokens.shape[0], w_query.shape[0]
    hidden, quarter = w_gate.shape
    lines, per = n // 2, n // n_mp
    step = max(128, -(-hidden // CHUNKS // 128) * 128)
    bounds = [
        (h, first, min(first + step, hidden))
        for h in range(HALVES)
        for first in range(0, hidden, step)
    ]
    part = rows // HALVES
    bf16, f32, dma = jnp.bfloat16, jnp.float32, pltpu.SemaphoreType.DMA
    scratch = dict(
        tokens=VMEM(tokens.shape, bf16),
        gain_attn=VMEM((1, D), f32),
        bias=VMEM((1, width), f32),
        gain_ffn=VMEM((1, width), f32),
        w_query=VMEM(w_query.shape, bf16),
        keys=VMEM(keys.shape, bf16),
        values=VMEM(keys.shape, bf16),
        w_out=VMEM((KV_HEADS, width, D // KV_HEADS), bf16),
        gate_w=VMEM(w_gate.shape, bf16),
        up_w=VMEM(w_gate.shape, bf16),
        down_w=VMEM(w_down.shape, bf16),
        own_tokens=VMEM((rows, width), f32),
        residual=VMEM((rows, width), f32),
        qbuf=VMEM((HALVES, n, part, width), bf16),
        part_out=VMEM((HALVES, n, part, width), bf16),
        part_in=VMEM((HALVES, n, part, width), bf16),
        stat_out=VMEM((HALVES, KV_HEADS, 2 * SUM_ROW, part), f32),
        stat_in=VMEM((HALVES, n, 2 * SUM_ROW, part), f32),
        att=VMEM((HALVES, n, part, width), bf16),
        lined=VMEM((HALVES, lines, part, width), bf16),
        squares=VMEM((HALVES, n, 1, part), f32),
        blocks=VMEM((HALVES, n_mp, per, part, width), bf16),
        features=VMEM((HALVES, n_mp * part, quarter), bf16),
        acc=VMEM((n_mp * part, w_down.shape[1]), f32),
        down_out=VMEM((HALVES, n_mp, 2, per // 2, part, width), bf16),
        home_in=VMEM((HALVES, 2, n_mp, per // 2, part, width), bf16),
        home_out=VMEM((HALVES, lines, part, width), bf16),
        terms=VMEM((HALVES, lines, part, width), bf16),
        w_sems=dma((10 + KV_HEADS,)),
        q_sems=dma((HALVES, 4, lines)),
        a_sems=dma((HALVES, 4, lines)),
        m_send=dma((HALVES, 2, n)),
        m_recv=dma((HALVES, 2, n)),
        l_sems=dma((HALVES, 2, lines)),
        sq_sems=dma((HALVES, 2, n)),
        r_send=dma((HALVES, 2, lines)),
        r_recv=dma((HALVES, n_mp, per)),
        h_sems=dma((HALVES, 2, 2 * n_mp)),
        t_send=dma((HALVES, lines)),
        t_recv=dma((HALVES, lines)),
        c_sems=dma((len(bounds), 10)),
    )
    for c, (_, first, last) in enumerate(bounds):
        span = last - first
        scratch[f"kept{c}"] = VMEM((2, 2, part, span), f32)
        scratch[f"s1_out{c}"] = VMEM((2, 2, part, span), bf16)
        scratch[f"s1_in{c}"] = VMEM((2, 2, part, span), bf16)
        scratch[f"s2_out{c}"] = VMEM((2, part, span), bf16)
        scratch[f"s2_in{c}"] = VMEM((2, part, span), bf16)
        scratch[f"act{c}"] = VMEM((n_mp, part, span), bf16)
    names = ARGS + OUTS + tuple(scratch)
    block = jax.ShapeDtypeStruct((rows, width), bf16)
    vmem, anywhere = pl.BlockSpec(memory_space=VMEM), pl.BlockSpec(memory_space=pl.ANY)
    return pl.pallas_call(
        functools.partial(layer_kernel, n, n_mp, bounds, names),
        out_shape=(block, block),
        in_specs=[anywhere] * len(ARGS),
        out_specs=(vmem, vmem),
        scratch_shapes=list(scratch.values()),
        compiler_params=pltpu.CompilerParams(
            collective_id=1, has_side_effects=True, vmem_limit_bytes=60 * 2**20
        ),
        name="layer",
    )(*arrays)


def body(
    n_seq,
    n_mp,
    tokens,
    gain_attn,
    w_query,
    query_bias,
    cache_keys,
    cache_values,
    w_out,
    gain_ffn,
    w_gate,
    w_up,
    w_down,
):
    return layer(
        n_seq,
        n_mp,
        tokens,
        gain_attn[None, :],
        w_query.T,
        query_bias[None, :],
        cache_keys,
        cache_values,
        w_out.T,
        gain_ffn[None, :],
        w_gate.T,
        w_up.T,
        w_down,
    )


def solution(mesh):
    placed = (
        P("mp", None),
        P(),
        P(None, "seq"),
        P("seq"),
        P(None, "seq", None),
        P(None, "seq", None),
        P(None, "seq"),
        P("seq"),
        P("mp", "seq"),
        P("mp", "seq"),
        P("seq", "mp"),
    )
    return jax.shard_map(
        functools.partial(body, mesh.shape["seq"], mesh.shape["mp"]),
        mesh=mesh,
        in_specs=placed,
        out_specs=(P("mp", "seq"), P("mp", "seq")),
        check_vma=False,
    )
```

```python
import functools
import math
import types

import jax
import jax.numpy as jnp
from jax import lax
from jax.experimental import pallas as pl
from jax.experimental.pallas import tpu as pltpu
from jax.sharding import PartitionSpec as P

D = 3584
HEADS = 28
KV_HEADS = 4
HEAD = 128
GROUP = HEADS // KV_HEADS
SUM_ROW = 8
CUTS = ((0.25, 0.6), (0.4, 0.75))
HALVES = 2
LAG = 2

eps = 1e-06
EXP2_SCALE = HEAD ** (-0.5) * math.log2(math.e)
MESH = pl.DeviceIdType.MESH
VMEM = pltpu.VMEM
ARGS = (
    "tokens_hbm", "gain_attn_hbm", "w_query_hbm", "bias_hbm", "keys_hbm", "values_hbm",
    "w_out_hbm", "gain_ffn_hbm", "gate_hbm", "up_hbm", "down_hbm",
)
OUTS = ("attended", "out")


def push(src, dst, send, recv, to):
    return pltpu.make_async_remote_copy(
        src_ref=src,
        dst_ref=dst,
        send_sem=send,
        recv_sem=recv,
        device_id=to,
        device_id_type=MESH,
    )


def times_transposed(a, b):
    return lax.dot_general(a, b, (((1,), (1,)), ((), ())), preferred_element_type=jnp.float32)


def row_to_column(row):
    k = row.shape[1]
    across = lax.broadcasted_iota(jnp.int32, (k, k), 1)
    down = lax.broadcasted_iota(jnp.int32, (k, k), 0)
    return jnp.sum(jnp.where(across == down, row, 0.0), axis=1, keepdims=True)


def column_to_row(column):
    k = column.shape[0]
    across = lax.broadcasted_iota(jnp.int32, (k, k), 1)
    down = lax.broadcasted_iota(jnp.int32, (k, k), 0)
    return jnp.sum(jnp.where(across == down, column, 0.0), axis=0, keepdims=True)


class Place:
    def __init__(self, n, n_mp):
        self.n, self.n_mp = n, n_mp
        self.lines, self.per, self.wide = n // 2, n // n_mp, n // KV_HEADS
        self.s, self.m = lax.axis_index("seq"), lax.axis_index("mp")
        self.hi, self.lo = self.s // 2, lax.rem(self.s, 2)
        self.y, self.core = self.m // 2, lax.rem(self.m, 2)
        self.partner = (self.hi * 2 + 1 - self.lo, self.m)
        self.sibling = (self.s, self.y * 2 + (1 - self.core))
        self.across = (self.s, (1 - self.y) * 2 + self.core)

    def ahead(self, d):
        return lax.rem(self.hi + d, self.lines)

    def behind(self, d):
        return lax.rem(self.hi + self.lines - d, self.lines)

    def near(self, b, m):
        return (self.hi * 2 + lax.rem(self.lo + b, 2), m)

    def group(self, j):
        return lax.rem(self.s // self.wide + KV_HEADS - j, KV_HEADS)


def greet(at):
    barrier = pltpu.get_barrier_semaphore()
    peers = [(lax.rem(at.s + d, at.n), at.m) for d in range(1, at.n)]
    peers += [
        at.near(b, lax.rem(at.m + i, at.n_mp)) for i in range(1, at.n_mp) for b in range(2)
    ]
    for peer in peers:
        pl.semaphore_signal(barrier, inc=1, device_id=peer, device_id_type=MESH)
    return lambda: pl.semaphore_wait(barrier, len(peers))


class Gather:
    def __init__(self, at, buf, sems, sent):
        self.at, self.buf, self.sems, self.sent = at, buf, sems, sent
        self.direct = [
            push(
                buf.at[at.s], buf.at[at.s], sent.sem, sems.at[0, d],
                (at.ahead(d) * 2 + at.lo, at.m),
            )
            for d in range(1, at.lines)
        ]
        self.handed, self.taken = [], 0

    def start(self):
        for copy in self.direct:
            copy.start()
            self.sent.count += 1
        self.hand(0)

    def hand(self, d):
        at = self.at
        if d < len(self.handed):
            return
        if d:
            self.direct[d - 1].wait_recv()
        block = self.buf.at[at.behind(d) * 2 + at.lo]
        copy = push(block, block, self.sent.sem, self.sems.at[1, d], at.partner)
        copy.start()
        self.handed.append(copy)
        self.sent.count += 1

    def hand_all(self):
        for d in range(self.at.lines):
            self.hand(d)

    def take(self, j):
        last = j if self.at.lines == KV_HEADS else self.at.lines - 1
        while self.taken <= last:
            self.hand(self.taken)
            self.handed[self.taken].wait_recv()
            self.taken += 1


class Sent:
    def __init__(self, sem, sized, to):
        self.sem, self.sized, self.to, self.count = sem, sized, to, 0

    def start(self, copy, blocks=1):
        copy.start()
        self.count += blocks

    def wait(self):
        of = self.sized.at[pl.ds(0, self.count)]
        push(of, of, self.sem, self.sem, self.to).wait_send()


def arrival(sized, count, sem, source):
    of = sized.at[pl.ds(0, count)]
    return push(of, of, sem, sem, source)


def layer_kernel(n, n_mp, bounds, names, *refs):
    R = types.SimpleNamespace(**dict(zip(names, refs)))
    at = Place(n, n_mp)
    s, m, hi, lo, y, core = at.s, at.m, at.hi, at.lo, at.y, at.core
    per, wide, lines = at.per, at.wide, at.lines
    rows, width = R.out.shape[0] // HALVES, R.out.shape[1]
    bf16, f32 = jnp.bfloat16, jnp.float32
    sent = Sent(R.s_sems.at[0], R.sized, at.partner)
    sent_stats = Sent(R.s_sems.at[1], R.sized_stats, at.partner)
    sent_squares = Sent(R.s_sems.at[2], R.sized_squares, at.partner)

    def part(h):
        return slice(h * rows, (h + 1) * rows)

    loads = {}
    slots = iter(range(R.w_sems.shape[0]))

    def load(name, src, dst):
        loads[name] = pltpu.make_async_copy(src, dst, R.w_sems.at[next(slots)])
        loads[name].start()

    load("tokens", R.tokens_hbm, R.tokens)
    load("gain_attn", R.gain_attn_hbm, R.gain_attn)
    load("bias", R.bias_hbm, R.bias)
    load("w_query", R.w_query_hbm, R.w_query)
    load("gain_ffn", R.gain_ffn_hbm, R.gain_ffn)
    everyone_here = greet(at)

    loads["tokens"].wait()
    hidden_in = R.tokens[...].astype(f32)
    mean_sq = jnp.sum(hidden_in * hidden_in, axis=1, keepdims=True) / D
    loads["gain_attn"].wait()
    normed = (hidden_in * lax.rsqrt(mean_sq + eps) * R.gain_attn[...].reshape(1, D)).astype(bf16)
    loads["bias"].wait()
    loads["w_query"].wait()
    load("keys", R.keys_hbm, R.keys)
    load("values", R.values_hbm, R.values)
    queries = (times_transposed(normed, R.w_query[...]) + R.bias[...]).astype(bf16)
    for h in range(HALVES):
        R.qbuf[h, s] = queries[part(h)]
    everyone_here()
    asked = [Gather(at, R.qbuf.at[h], R.q_sems.at[h], sent) for h in range(HALVES)]
    for flow in asked:
        flow.start()
    span = D // KV_HEADS
    for g in range(KV_HEADS):
        load(f"w_out{g}", R.w_out_hbm.at[:, pl.ds(g * span, span)], R.w_out.at[g])
    load("gate", R.gate_hbm, R.gate_w)
    load("up", R.up_hbm, R.up_w)
    load("down", R.down_hbm, R.down_w)
    for k in range(n):

        @pl.when(s == k)
        def _():
            R.own_tokens[...] = R.tokens[:, k * width : (k + 1) * width].astype(f32)

    def attend(h, j):
        g = at.group(j)
        q = jnp.concatenate([R.qbuf[h, g * wide + i] for i in range(wide)], axis=1)
        stacked = jnp.concatenate([q[:, i * HEAD : (i + 1) * HEAD] for i in range(GROUP)], axis=0)
        scores = times_transposed(stacked, R.keys[g])
        highest = jnp.max(scores, axis=1, keepdims=True)
        probs = jnp.exp2((scores - highest) * EXP2_SCALE)
        sums = jnp.sum(probs, axis=1, keepdims=True)
        weighted = jnp.dot(probs.astype(bf16), R.values[g], preferred_element_type=f32)
        side = jnp.concatenate([weighted[part(i)] for i in range(GROUP)], axis=1).astype(bf16)
        for i in range(wide):
            R.part_out[h, j, i % 2, i // 2] = side[:, i * width : (i + 1) * width]
        R.stat_out[h, j] = jnp.zeros((2 * SUM_ROW, rows), f32)
        for i in range(GROUP):
            R.stat_out[h, j, i : i + 1, :] = column_to_row(highest[part(i)] * EXP2_SCALE)
            R.stat_out[h, j, i + SUM_ROW : i + SUM_ROW + 1, :] = column_to_row(sums[part(i)])
        for src, dst, k, record, blocks in (
            (R.part_out.at[h, j, 1 - lo], R.pair_in.at[h, j], 0, sent, wide // 2),
            (R.stat_out.at[h, j], R.pair_stat.at[h, j], 1, sent_stats, 1),
        ):
            copy = push(src, dst, record.sem, R.p_sems.at[h, k, j], at.partner)
            record.start(copy, blocks)
            paired[h, j].append(copy)

    paired = {(h, j): [] for h in range(HALVES) for j in range(KV_HEADS)}
    index = lax.rem(lax.broadcasted_iota(jnp.int32, (2 * SUM_ROW, width), 0), SUM_ROW)
    picks = []
    for k in range(wide // 2):
        first = (k * 2 + lo) * width
        column = first + lax.broadcasted_iota(jnp.int32, (2 * SUM_ROW, width), 1)
        picks.append(jnp.where(lax.div(column, HEAD) == index, 1.0, 0.0).astype(bf16))

    def spread(factor, pick):
        coarse = factor.astype(bf16).astype(f32)
        pair = jnp.concatenate([coarse, factor - coarse], axis=0).astype(bf16)
        return lax.dot_general(pair, pick, (((0,), (0,)), ((), ())), preferred_element_type=f32)

    def join(h, j):
        for copy in paired[h, j]:
            copy.wait_recv()
        mine, other = R.stat_out[h, j], R.pair_stat[h, j]
        top = jnp.maximum(mine[:SUM_ROW], other[:SUM_ROW])
        scale, scale_other = jnp.exp2(mine[:SUM_ROW] - top), jnp.exp2(other[:SUM_ROW] - top)
        R.line_stat[h, j, :SUM_ROW, :] = top
        R.line_stat[h, j, SUM_ROW:, :] = mine[SUM_ROW:] * scale + other[SUM_ROW:] * scale_other
        g = at.group(j)
        for k in range(wide // 2):
            total = R.part_out[h, j, lo, k].astype(f32) * spread(scale, picks[k]) + R.pair_in[
                h, j, k
            ].astype(f32) * spread(scale_other, picks[k])
            R.line_out[h, j, k] = total.astype(bf16)
            line = g * (wide // 2) + k
            if wide // 2 == 1 and j == 0:
                R.part_in[h, hi] = R.line_out[h, j, k]
                R.stat_in[h, hi] = R.line_stat[h, j]
                continue
            for src, dst, kind, record in (
                (R.line_out.at[h, j, k], R.part_in.at[h, hi], 0, sent),
                (R.line_stat.at[h, j], R.stat_in.at[h, hi], 1, sent_stats),
            ):
                copy = push(src, dst, record.sem, R.m_recv.at[h, kind], (line * 2 + lo, m))
                if j:
                    record.start(copy)
                    continue

                @pl.when(line != hi)
                def _():
                    copy.start()

                record.count += int(k > 0)
            if j == 0:

                @pl.when(line == hi)
                def _():
                    R.part_in[h, hi] = R.line_out[h, j, k]
                    R.stat_in[h, hi] = R.line_stat[h, j]

    def merge(h):
        arrival(R.sized, lines - 1, R.m_recv.at[h, 0], at.partner).wait_recv()
        arrival(R.sized_stats, lines - 1, R.m_recv.at[h, 1], at.partner).wait_recv()
        maxima, sums = R.stat_in[h, :, :SUM_ROW, :], R.stat_in[h, :, SUM_ROW:, :]
        rescale = jnp.exp2(maxima - jnp.max(maxima, axis=0, keepdims=True))
        total = jnp.sum(sums * rescale, axis=0)
        row = lax.broadcasted_iota(jnp.int32, (SUM_ROW, rows), 0)
        inverse = 1.0 / jnp.where(row < GROUP, total, 1.0)
        column = lax.rem(s, wide) * width + lax.broadcasted_iota(
            jnp.int32, (2 * SUM_ROW, width), 1
        )
        pick = jnp.where(lax.div(column, HEAD) == index, 1.0, 0.0).astype(bf16)
        result = jnp.zeros((rows, width), f32)
        for i in range(lines):
            result = result + R.part_in[h, i].astype(f32) * spread(rescale[i] * inverse, pick)
        R.att[h, s] = result.astype(bf16)
        copy = pltpu.make_async_copy(R.att.at[h, s], R.attended.at[pl.ds(h * rows, rows)], R.o_sems.at[0, h])
        copy.start()
        written.append(copy)

    written = []

    def project(h, flow):
        total = R.own_tokens[part(h), :]
        for j in range(KV_HEADS):
            flow.take(j)
            g = at.group(j)
            block = jnp.concatenate([R.att[h, g * wide + i] for i in range(wide)], axis=1)
            total = total + times_transposed(block, R.w_out[g])
        R.residual[part(h), :] = total
        R.lined[h, hi] = (total * R.gain_ffn[...]).astype(bf16)
        R.squares[h, s] = column_to_row(jnp.sum(total * total, axis=1, keepdims=True))
        for d in range(1, lines):
            copy = push(
                R.lined.at[h, hi], R.lined.at[h, hi], sent.sem, R.l_sems.at[h, d],
                (at.ahead(d) * 2 + lo, m),
            )
            sent.start(copy)
            lined[h].append(copy)
        relay(h, range(1))
        for d in range(1, n):
            copy = push(
                R.squares.at[h, s], R.squares.at[h, s], sent_squares.sem, R.sq_sems.at[h],
                (lax.rem(s + d, n), m),
            )
            sent_squares.start(copy)

    lined = [[] for _ in range(HALVES)]

    def relay(h, steps):
        for d in steps:
            if d:
                lined[h][d - 1].wait_recv()
            line = at.behind(d)
            source = line * 2 + lo
            to_m, k = source // per, lax.rem(source, per)
            for b in range(2):
                copy = push(
                    R.lined.at[h, line], R.blocks.at[h, m, k], sent.sem, R.r_recv.at[h],
                    at.near(b, to_m),
                )
                if b:
                    sent.start(copy)
                    continue

                @pl.when(to_m == m)
                def _():
                    R.blocks[h, m, k] = R.lined[h, line]

                @pl.when(to_m != m)
                def _():
                    copy.start()

        if 0 in steps:
            sent.count += lines - per // 2

    order = (1 - core, 3 - core, core, 2 + core)

    def collect(h):
        arrival(R.sized, n_mp * per - per // 2, R.r_recv.at[h], at.partner).wait_recv()
        for p, t in enumerate(order):
            R.features[h, p * rows : (p + 1) * rows, :] = jnp.concatenate(
                [R.blocks[h, t, j] for j in range(per)], axis=1
            )

    def inverse_of(h):
        arrival(R.sized_squares, n - 1, R.sq_sems.at[h], at.partner).wait_recv()
        return row_to_column(lax.rsqrt(jnp.sum(R.squares[h], axis=0) / D + eps))

    chunks = []
    for c, (h, first, last) in enumerate(bounds):
        kept, s1_out, s1_in, s2_out, s2_in, act = (
            getattr(R, f"{name}{c}") for name in ("kept", "s1_out", "s1_in", "s2_out", "s2_in", "act")
        )
        sem = lambda k, c=c: R.c_sems.at[c, k]
        chunks.append(
            dict(
                half=h, first=first, last=last, kept=kept, s1_out=s1_out, s1_in=s1_in,
                s2_out=s2_out, s2_in=s2_in, act=act,
                s1=push(s1_out, s1_in, sem(0), sem(1), at.sibling),
                s2=push(s2_out, s2_in, sem(0), sem(2), at.across),
                near=push(act.at[m], act.at[m], sem(0), sem(3), at.sibling),
                far=push(act.at[m], act.at[m], sem(0), sem(4), at.across),
                relay=push(
                    act.at[at.across[1]], act.at[at.across[1]], sem(0), sem(5), at.sibling
                ),
                sent=Sent(sem(0), getattr(R, f"sized{c}"), at.partner),
            )
        )
    halves = [[ch for ch in chunks if ch["half"] == h] for h in range(HALVES)]

    def multiply(ch):
        for g, weight in enumerate((R.gate_w, R.up_w)):
            product = times_transposed(R.features[ch["half"]], weight[ch["first"] : ch["last"], :])
            for p in range(2):
                ch["s1_out"][g, p] = product[p * rows : (p + 1) * rows].astype(bf16)
                ch["kept"][g, p] = product[(p + 2) * rows : (p + 3) * rows]
        ch["s1"].start()

    def pair_sum(ch):
        ch["s1"].wait_recv()
        for g in range(2):
            ch["s2_out"][g] = (
                ch["kept"][g, 1 - y] + ch["s1_in"][g, 1 - y].astype(f32)
            ).astype(bf16)
        ch["s2"].start()

    def activate(ch, inverse):
        ch["s2"].wait_recv()
        gate, up = [
            (ch["kept"][g, y] + ch["s1_in"][g, y].astype(f32) + ch["s2_in"][g].astype(f32))
            * inverse
            for g in range(2)
        ]
        ch["act"][m] = (gate / (1.0 + jnp.exp(-gate)) * up).astype(bf16)
        ch["far"].start()
        ch["near"].start()

    def pass_on(ch):
        ch["far"].wait_recv()
        ch["relay"].start()

    def down(ch):
        h, own = ch["half"], halves[ch["half"]]
        ch["near"].wait_recv()
        ch["relay"].wait_recv()
        act = ch["act"][...].reshape(n_mp * rows, ch["last"] - ch["first"])
        total = jnp.dot(act, R.down_w[ch["first"] : ch["last"], :], preferred_element_type=f32)
        if ch is not own[0]:
            total = R.acc[h] + total
        if ch is not own[-1]:
            R.acc[h] = total
            return
        for t in range(n_mp):
            for k in range(per):
                R.down_out[h, t, k % 2, k // 2] = total[
                    t * rows : (t + 1) * rows, k * width : (k + 1) * width
                ].astype(bf16)

    def leave(h):
        for i in range(n_mp):
            for b in range(2):
                if i == 0 and b == 0:
                    R.home_in[h, lo, m] = R.down_out[h, m, lo]
                    continue
                to_m, to_lo = lax.rem(m + i, n_mp), lax.rem(lo + b, 2)
                copy = push(
                    R.down_out.at[h, to_m, to_lo], R.home_in.at[h, lo, m], sent.sem,
                    R.h_sems.at[h, i], at.near(b, to_m),
                )
                sent.start(copy, per // 2)


    def send_home(h):
        for i in range(n_mp):
            source = lax.rem(m + n_mp - i, n_mp)
            blocks = (2 if i else 1) * (per // 2)
            arrival(R.sized, blocks, R.h_sems.at[h, i], at.partner).wait_recv()
            for k in range(per // 2):
                line = source * (per // 2) + k
                total = R.home_in[h, 0, source, k].astype(f32) + R.home_in[h, 1, source, k].astype(f32)
                R.home_out[h, line] = total.astype(bf16)
                copy = push(
                    R.home_out.at[h, line], R.terms.at[h, hi], sent.sem, R.t_recv.at[h],
                    (line * 2 + lo, m),
                )

                @pl.when(line == hi)
                def _():
                    R.terms[h, hi] = R.home_out[h, line]

                @pl.when(line != hi)
                def _():
                    copy.start()

        sent.count += lines - 1

    def conclude(h):
        arrival(R.sized, lines - 1, R.t_recv.at[h], at.partner).wait_recv()
        result = R.residual[part(h), :]
        for i in range(lines):
            result = result + R.terms[h, i].astype(f32)
        R.result[part(h), :] = result.astype(bf16)
        copy = pltpu.make_async_copy(
            R.result.at[pl.ds(h * rows, rows)], R.out.at[pl.ds(h * rows, rows)], R.o_sems.at[1, h]
        )
        copy.start()
        written.append(copy)

    loads["keys"].wait()
    loads["values"].wait()
    waiting = []
    for h in range(HALVES):
        for j in range(KV_HEADS):
            asked[h].take(j)
            attend(h, j)
            if h == 0 and j == 0:
                asked[0].hand_all()
            elif h + 1 < HALVES and lines == KV_HEADS:
                asked[h + 1].hand(j)
            waiting.append((h, j))
            if len(waiting) > LAG:
                join(*waiting.pop(0))
        if h + 1 < HALVES:
            asked[h + 1].hand_all()
    for item in waiting:
        join(*item)
    for g in range(KV_HEADS):
        loads[f"w_out{g}"].wait()
    loads["gain_ffn"].wait()
    answered = [Gather(at, R.att.at[h], R.a_sems.at[h], sent) for h in range(HALVES)]
    for h in range(HALVES):
        merge(h)
        answered[h].start()
    first, second = halves
    answered[0].hand_all()
    project(0, answered[0])
    answered[1].hand_all()
    project(1, answered[1])
    loads["gate"].wait()
    loads["up"].wait()
    later = range(1, lines)
    relay(0, later)
    collect(0)
    multiply(first[0])
    relay(1, later)
    pair_sum(first[0])
    for ch in first[1:]:
        multiply(ch)
        pair_sum(ch)
    inverse = [inverse_of(0)]
    collect(1)
    loads["down"].wait()
    for k, ch in enumerate(second):
        multiply(ch)
        activate(first[k], inverse[0])
        pair_sum(ch)
    inverse.append(inverse_of(1))
    for k, ch in enumerate(second):
        pass_on(first[k])
        down(first[k])
        activate(ch, inverse[1])
    leave(0)
    for ch in second:
        pass_on(ch)
        down(ch)
    leave(1)
    send_home(0)
    send_home(1)
    for h in range(HALVES):
        conclude(h)

    for copy in written:
        copy.wait()
    for record in (sent, sent_stats, sent_squares):
        record.wait()
    for ch in chunks:
        ch["sent"].count = 9
        ch["sent"].wait()


def layer(n, n_mp, *arrays):
    tokens, w_query, keys, w_gate, w_down = (arrays[i] for i in (0, 2, 4, 8, 10))
    rows, width = tokens.shape[0], w_query.shape[0]
    hidden, quarter = w_gate.shape
    lines, per = n // 2, n // n_mp
    bounds = []
    for h in range(HALVES):
        cuts = [min(hidden, -(-int(hidden * cut) // 128) * 128) for cut in CUTS[h]] + [hidden]
        bounds += [(h, first, last) for first, last in zip([0] + cuts, cuts) if first < last]
    part = rows // HALVES
    bf16, f32, dma = jnp.bfloat16, jnp.float32, pltpu.SemaphoreType.DMA
    scratch = dict(
        tokens=VMEM(tokens.shape, bf16),
        gain_attn=VMEM((D,), f32),
        bias=VMEM((1, width), f32),
        gain_ffn=VMEM((1, width), f32),
        w_query=VMEM(w_query.shape, bf16),
        keys=VMEM(keys.shape, bf16),
        values=VMEM(keys.shape, bf16),
        w_out=VMEM((KV_HEADS, width, D // KV_HEADS), bf16),
        gate_w=VMEM(w_gate.shape, bf16),
        up_w=VMEM(w_gate.shape, bf16),
        down_w=VMEM(w_down.shape, bf16),
        own_tokens=VMEM((rows, width), f32),
        residual=VMEM((rows, width), f32),
        qbuf=VMEM((HALVES, n, part, width), bf16),
        part_out=VMEM((HALVES, KV_HEADS, 2, n // KV_HEADS // 2, part, width), bf16),
        pair_in=VMEM((HALVES, KV_HEADS, n // KV_HEADS // 2, part, width), bf16),
        line_out=VMEM((HALVES, KV_HEADS, n // KV_HEADS // 2, part, width), bf16),
        part_in=VMEM((HALVES, lines, part, width), bf16),
        stat_out=VMEM((HALVES, KV_HEADS, 2 * SUM_ROW, part), f32),
        pair_stat=VMEM((HALVES, KV_HEADS, 2 * SUM_ROW, part), f32),
        line_stat=VMEM((HALVES, KV_HEADS, 2 * SUM_ROW, part), f32),
        stat_in=VMEM((HALVES, lines, 2 * SUM_ROW, part), f32),
        result=VMEM((rows, width), bf16),
        att=VMEM((HALVES, n, part, width), bf16),
        lined=VMEM((HALVES, lines, part, width), bf16),
        squares=VMEM((HALVES, n, 1, part), f32),
        blocks=VMEM((HALVES, n_mp, per, part, width), bf16),
        features=VMEM((HALVES, n_mp * part, quarter), bf16),
        acc=VMEM((HALVES, n_mp * part, w_down.shape[1]), f32),
        down_out=VMEM((HALVES, n_mp, 2, per // 2, part, width), bf16),
        home_in=VMEM((HALVES, 2, n_mp, per // 2, part, width), bf16),
        home_out=VMEM((HALVES, lines, part, width), bf16),
        terms=VMEM((HALVES, lines, part, width), bf16),
        sized=VMEM((HALVES * 8 * n, part, width), bf16),
        sized_stats=VMEM((HALVES * 2 * n, 2 * SUM_ROW, part), f32),
        sized_squares=VMEM((HALVES * n, 1, part), f32),
        w_sems=dma((10 + KV_HEADS,)),
        s_sems=dma((3,)),
        q_sems=dma((HALVES, 2, lines)),
        a_sems=dma((HALVES, 2, lines)),
        p_sems=dma((HALVES, 2, KV_HEADS)),
        m_recv=dma((HALVES, 2)),
        o_sems=dma((2, HALVES)),
        l_sems=dma((HALVES, lines)),
        sq_sems=dma((HALVES,)),
        r_recv=dma((HALVES,)),
        h_sems=dma((HALVES, n_mp)),
        t_recv=dma((HALVES,)),
        c_sems=dma((len(bounds), 6)),
    )
    for c, (_, first, last) in enumerate(bounds):
        span = last - first
        scratch[f"kept{c}"] = VMEM((2, 2, part, span), f32)
        scratch[f"s1_out{c}"] = VMEM((2, 2, part, span), bf16)
        scratch[f"s1_in{c}"] = VMEM((2, 2, part, span), bf16)
        scratch[f"s2_out{c}"] = VMEM((2, part, span), bf16)
        scratch[f"s2_in{c}"] = VMEM((2, part, span), bf16)
        scratch[f"sized{c}"] = VMEM((9, part, span), bf16)
        scratch[f"act{c}"] = VMEM((n_mp, part, span), bf16)
    names = ARGS + OUTS + tuple(scratch)
    block = jax.ShapeDtypeStruct((rows, width), bf16)
    anywhere = pl.BlockSpec(memory_space=pl.ANY)
    return pl.pallas_call(
        functools.partial(layer_kernel, n, n_mp, bounds, names),
        out_shape=(block, block),
        in_specs=[anywhere] * len(ARGS),
        out_specs=(anywhere, anywhere),
        scratch_shapes=list(scratch.values()),
        compiler_params=pltpu.CompilerParams(
            collective_id=1, has_side_effects=True, vmem_limit_bytes=60 * 2**20
        ),
        name="layer",
    )(*arrays)


def results_kernel(attended, out, attended_out, layer_out, held, sems):
    pairs = ((attended, attended_out), (out, layer_out))
    into = [pltpu.make_async_copy(src, held.at[i], sems.at[0, i]) for i, (src, _) in enumerate(pairs)]
    back = [pltpu.make_async_copy(held.at[i], dst, sems.at[1, i]) for i, (_, dst) in enumerate(pairs)]
    for copy in into:
        copy.start()
    for copy, onward in zip(into, back):
        copy.wait()
        onward.start()
    for copy in back:
        copy.wait()


def results(attended, out):
    anywhere = pl.BlockSpec(memory_space=pl.ANY)
    block = jax.ShapeDtypeStruct(out.shape, out.dtype)
    return pl.pallas_call(
        results_kernel,
        out_shape=(block, block),
        in_specs=[anywhere, anywhere],
        out_specs=(anywhere, anywhere),
        scratch_shapes=[VMEM((2,) + out.shape, out.dtype), pltpu.SemaphoreType.DMA((2, 2))],
        name="results",
    )(attended, out)


def body(
    n_seq,
    n_mp,
    tokens,
    gain_attn,
    w_query,
    query_bias,
    cache_keys,
    cache_values,
    w_out,
    gain_ffn,
    w_gate,
    w_up,
    w_down,
):
    attended, out = layer(
        n_seq,
        n_mp,
        tokens,
        gain_attn,
        w_query.T,
        query_bias[None, :],
        cache_keys,
        cache_values,
        w_out.T,
        gain_ffn[None, :],
        w_gate.T,
        w_up.T,
        w_down,
    )
    return results(attended, out)


def solution(mesh):
    placed = (
        P("mp", None),
        P(),
        P(None, "seq"),
        P("seq"),
        P(None, "seq", None),
        P(None, "seq", None),
        P(None, "seq"),
        P("seq"),
        P("mp", "seq"),
        P("mp", "seq"),
        P("seq", "mp"),
    )
    return jax.shard_map(
        functools.partial(body, mesh.shape["seq"], mesh.shape["mp"]),
        mesh=mesh,
        in_specs=placed,
        out_specs=(P("mp", "seq"), P("mp", "seq")),
        check_vma=False,
    )
```

```python
import functools
import math
import types

import jax
import jax.numpy as jnp
from jax import lax
from jax.experimental import pallas as pl
from jax.experimental.pallas import tpu as pltpu
from jax.sharding import PartitionSpec as P

D = 3584
HEADS = 28
KV_HEADS = 4
HEAD = 128
GROUP = HEADS // KV_HEADS
SUM_ROW = 8
CUTS = ((0.3, 0.65), (0.45, 0.82))
PARTS = 2
ROWS = (0.5, 0.5)
LAG = 2
FORWARD = (False, False)
ASK_STRAIGHT = (True, False)
ANSWER_STRAIGHT = (False, False)

eps = 1e-06
EXP2_SCALE = HEAD ** (-0.5) * math.log2(math.e)
MESH = pl.DeviceIdType.MESH
VMEM = pltpu.VMEM
ARGS = (
    "tokens_hbm", "gain_attn_hbm", "w_query_hbm", "bias_hbm", "keys_hbm", "values_hbm",
    "w_out_hbm", "gain_ffn_hbm", "gate_hbm", "up_hbm", "down_hbm",
)
OUTS = ("attended", "out")


def push(src, dst, send, recv, to):
    return pltpu.make_async_remote_copy(
        src_ref=src,
        dst_ref=dst,
        send_sem=send,
        recv_sem=recv,
        device_id=to,
        device_id_type=MESH,
    )


def times_transposed(a, b):
    return lax.dot_general(a, b, (((1,), (1,)), ((), ())), preferred_element_type=jnp.float32)


def row_to_column(row):
    k = row.shape[1]
    across = lax.broadcasted_iota(jnp.int32, (k, k), 1)
    down = lax.broadcasted_iota(jnp.int32, (k, k), 0)
    return jnp.sum(jnp.where(across == down, row, 0.0), axis=1, keepdims=True)


def column_to_row(column):
    k = column.shape[0]
    across = lax.broadcasted_iota(jnp.int32, (k, k), 1)
    down = lax.broadcasted_iota(jnp.int32, (k, k), 0)
    return jnp.sum(jnp.where(across == down, column, 0.0), axis=0, keepdims=True)


def part_rows(rows):
    sizes = [int(rows * share) for share in ROWS]
    return [sum(sizes[:h]) for h in range(PARTS)], sizes


class Place:
    def __init__(self, n, n_mp):
        self.n, self.n_mp = n, n_mp
        self.lines, self.per, self.wide = n // 2, n // n_mp, n // KV_HEADS
        self.s, self.m = lax.axis_index("seq"), lax.axis_index("mp")
        self.hi, self.lo = self.s // 2, lax.rem(self.s, 2)
        self.y, self.core = self.m // 2, lax.rem(self.m, 2)
        self.partner = (self.hi * 2 + 1 - self.lo, self.m)
        self.sibling = (self.s, self.y * 2 + (1 - self.core))
        self.across = (self.s, (1 - self.y) * 2 + self.core)

    def ahead(self, d):
        return lax.rem(self.hi + d, self.lines)

    def behind(self, d):
        return lax.rem(self.hi + self.lines - d, self.lines)

    def near(self, b, m):
        return (self.hi * 2 + lax.rem(self.lo + b, 2), m)

    def group(self, j):
        return lax.rem(self.s // self.wide + KV_HEADS - j, KV_HEADS)


def greet(at):
    barrier = pltpu.get_barrier_semaphore()
    peers = [(lax.rem(at.s + d, at.n), at.m) for d in range(1, at.n)]
    peers += [
        at.near(b, lax.rem(at.m + i, at.n_mp)) for i in range(1, at.n_mp) for b in range(2)
    ]
    for peer in peers:
        pl.semaphore_signal(barrier, inc=1, device_id=peer, device_id_type=MESH)
    return lambda: pl.semaphore_wait(barrier, len(peers))


class Gather:
    def __init__(self, at, buf, sems, sent, straight):
        self.at, self.buf, self.sems, self.sent = at, buf, sems, sent
        self.straight = straight
        self.direct = [
            push(
                buf.at[at.s], buf.at[at.s], sent.sem, sems.at[d - 1],
                (at.ahead(d) * 2 + at.lo, at.m),
            )
            for d in range(1, at.lines)
        ]
        self.handed, self.taken = [], 0

    def start(self):
        at = self.at
        for copy in self.direct:
            copy.start()
            self.sent.count += 1
        self.hand(0)
        for d in range(1, at.lines if self.straight else 1):
            copy = push(
                self.buf.at[at.s], self.buf.at[at.s], self.sent.sem,
                self.sems.at[at.lines - 1 + d], (at.ahead(d) * 2 + 1 - at.lo, at.m),
            )

            @pl.when(at.core == 0)
            def _():
                copy.start()


    def hand(self, d):
        at = self.at
        if d < len(self.handed):
            return
        if d:
            self.direct[d - 1].wait_recv()
        block = self.buf.at[at.behind(d) * 2 + at.lo]
        copy = push(block, block, self.sent.sem, self.sems.at[at.lines - 1 + d], at.partner)
        if d and self.straight:

            @pl.when(at.core != 0)
            def _():
                copy.start()

        else:
            copy.start()
        self.handed.append(copy)
        self.sent.count += 1

    def hand_all(self):
        for d in range(self.at.lines):
            self.hand(d)

    def take(self, j):
        last = j if self.at.lines == KV_HEADS else self.at.lines - 1
        while self.taken <= last:
            self.hand(self.taken)
            self.handed[self.taken].wait_recv()
            self.taken += 1


class Sent:
    def __init__(self, sem, sized, to):
        self.sem, self.sized, self.to, self.count = sem, sized, to, 0

    def start(self, copy, blocks=1):
        copy.start()
        self.count += blocks

    def wait(self):
        of = self.sized.at[pl.ds(0, self.count)]
        push(of, of, self.sem, self.sem, self.to).wait_send()


def arrival(sized, count, sem, source):
    of = sized.at[pl.ds(0, count)]
    return push(of, of, sem, sem, source)


def layer_kernel(n, n_mp, bounds, per_part, names, *refs):
    R = types.SimpleNamespace(**dict(zip(names, refs)))
    at = Place(n, n_mp)
    s, m, hi, lo, y, core = at.s, at.m, at.hi, at.lo, at.y, at.core
    per, wide, lines = at.per, at.wide, at.lines
    width = R.out.shape[1]
    for name in per_part:
        setattr(R, name, [getattr(R, f"{name}_{h}") for h in range(PARTS)])
    bf16, f32 = jnp.bfloat16, jnp.float32
    starts, sizes = part_rows(R.out.shape[0])
    sent, sent_stats, sent_squares = (
        [Sent(R.s_sems.at[k, h], sized[h], at.partner) for h in range(PARTS)]
        for k, sized in enumerate((R.sized, R.sized_stats, R.sized_squares))
    )

    def part(h):
        return slice(starts[h], starts[h] + sizes[h])

    loads = {}
    slots = iter(range(R.w_sems.shape[0]))

    def load(name, src, dst):
        loads[name] = pltpu.make_async_copy(src, dst, R.w_sems.at[next(slots)])
        loads[name].start()

    load("tokens", R.tokens_hbm, R.tokens)
    load("gain_attn", R.gain_attn_hbm, R.gain_attn)
    load("bias", R.bias_hbm, R.bias)
    span = D // KV_HEADS
    for g in range(KV_HEADS):
        load(f"w_query{g}", R.w_query_hbm.at[:, pl.ds(g * span, span)], R.w_query.at[g])
    load("gain_ffn", R.gain_ffn_hbm, R.gain_ffn)
    everyone_here = greet(at)

    loads["tokens"].wait()
    hidden_in = R.tokens[...].astype(f32)
    mean_sq = jnp.sum(hidden_in * hidden_in, axis=1, keepdims=True) / D
    loads["gain_attn"].wait()
    normed = (hidden_in * lax.rsqrt(mean_sq + eps) * R.gain_attn[...].reshape(1, D)).astype(bf16)
    loads["bias"].wait()
    total = R.bias[...]
    for g in range(KV_HEADS):
        loads[f"w_query{g}"].wait()
        if g == KV_HEADS - 1:
            load("keys", R.keys_hbm, R.keys)
            load("values", R.values_hbm, R.values)
        total = total + times_transposed(normed[:, g * span : (g + 1) * span], R.w_query[g])
    queries = total.astype(bf16)
    for h in range(PARTS):
        R.qbuf[h][s] = queries[part(h)]
    everyone_here()
    asked = [Gather(at, R.qbuf[h], R.q_sems.at[h], sent[h], ASK_STRAIGHT[h]) for h in range(PARTS)]
    for flow in asked:
        flow.start()
    for g in range(KV_HEADS):
        load(f"w_out{g}", R.w_out_hbm.at[:, pl.ds(g * span, span)], R.w_out.at[g])
    load("gate", R.gate_hbm, R.gate_w)
    load("up", R.up_hbm, R.up_w)
    load("down", R.down_hbm, R.down_w)
    for k in range(n):

        @pl.when(s == k)
        def _():
            R.own_tokens[...] = R.tokens[:, k * width : (k + 1) * width].astype(f32)

    def attend(h, j):
        g, rows = at.group(j), sizes[h]
        heads = [slice(i * rows, (i + 1) * rows) for i in range(GROUP)]
        q = jnp.concatenate([R.qbuf[h][g * wide + i] for i in range(wide)], axis=1)
        stacked = jnp.concatenate([q[:, i * HEAD : (i + 1) * HEAD] for i in range(GROUP)], axis=0)
        scores = times_transposed(stacked, R.keys[g])
        highest = jnp.max(scores, axis=1, keepdims=True)
        probs = jnp.exp2((scores - highest) * EXP2_SCALE)
        sums = jnp.sum(probs, axis=1, keepdims=True)
        weighted = jnp.dot(probs.astype(bf16), R.values[g], preferred_element_type=f32)
        side = jnp.concatenate([weighted[head] for head in heads], axis=1).astype(bf16)
        for i in range(wide):
            R.part_out[h][j, i % 2, i // 2] = side[:, i * width : (i + 1) * width]
        R.stat_out[h][j] = jnp.zeros((2 * SUM_ROW, rows), f32)
        for i in range(GROUP):
            R.stat_out[h][j, i : i + 1, :] = column_to_row(highest[heads[i]] * EXP2_SCALE)
            R.stat_out[h][j, i + SUM_ROW : i + SUM_ROW + 1, :] = column_to_row(sums[heads[i]])
        for src, dst, k, record, blocks in (
            (R.part_out[h].at[j, 1 - lo], R.pair_in[h].at[j], 0, sent[h], wide // 2),
            (R.stat_out[h].at[j], R.pair_stat[h].at[j], 1, sent_stats[h], 1),
        ):
            copy = push(src, dst, record.sem, R.p_sems.at[h, k, j], at.partner)
            record.start(copy, blocks)
            paired[h, j].append(copy)

    paired = {(h, j): [] for h in range(PARTS) for j in range(KV_HEADS)}
    index = lax.rem(lax.broadcasted_iota(jnp.int32, (2 * SUM_ROW, width), 0), SUM_ROW)
    picks = []
    for k in range(wide // 2):
        first = (k * 2 + lo) * width
        column = first + lax.broadcasted_iota(jnp.int32, (2 * SUM_ROW, width), 1)
        picks.append(jnp.where(lax.div(column, HEAD) == index, 1.0, 0.0).astype(bf16))

    def spread(factor, pick):
        coarse = factor.astype(bf16).astype(f32)
        pair = jnp.concatenate([coarse, factor - coarse], axis=0).astype(bf16)
        return lax.dot_general(pair, pick, (((0,), (0,)), ((), ())), preferred_element_type=f32)

    def join(h, j):
        for copy in paired[h, j]:
            copy.wait_recv()
        mine, other = R.stat_out[h][j], R.pair_stat[h][j]
        top = jnp.maximum(mine[:SUM_ROW], other[:SUM_ROW])
        scale, scale_other = jnp.exp2(mine[:SUM_ROW] - top), jnp.exp2(other[:SUM_ROW] - top)
        R.line_stat[h][j, :SUM_ROW, :] = top
        R.line_stat[h][j, SUM_ROW:, :] = mine[SUM_ROW:] * scale + other[SUM_ROW:] * scale_other
        g = at.group(j)
        for k in range(wide // 2):
            total = R.part_out[h][j, lo, k].astype(f32) * spread(scale, picks[k]) + R.pair_in[h][j, k].astype(f32) * spread(scale_other, picks[k])
            R.line_out[h][j, k] = total.astype(bf16)
            line = g * (wide // 2) + k
            if wide // 2 == 1 and j == 0:
                R.part_in[h][hi] = R.line_out[h][j, k]
                R.stat_in[h][hi] = R.line_stat[h][j]
                continue
            for src, dst, kind, record in (
                (R.line_out[h].at[j, k], R.part_in[h].at[hi], 0, sent[h]),
                (R.line_stat[h].at[j], R.stat_in[h].at[hi], 1, sent_stats[h]),
            ):
                copy = push(src, dst, record.sem, R.m_recv.at[h, kind], (line * 2 + lo, m))
                if j:
                    record.start(copy)
                    continue

                @pl.when(line != hi)
                def _():
                    copy.start()

                record.count += int(k > 0)
            if j == 0:

                @pl.when(line == hi)
                def _():
                    R.part_in[h][hi] = R.line_out[h][j, k]
                    R.stat_in[h][hi] = R.line_stat[h][j]

    def merge(h):
        rows = sizes[h]
        arrival(R.sized[h], lines - 1, R.m_recv.at[h, 0], at.partner).wait_recv()
        arrival(R.sized_stats[h], lines - 1, R.m_recv.at[h, 1], at.partner).wait_recv()
        maxima, sums = R.stat_in[h][:, :SUM_ROW, :], R.stat_in[h][:, SUM_ROW:, :]
        rescale = jnp.exp2(maxima - jnp.max(maxima, axis=0, keepdims=True))
        total = jnp.sum(sums * rescale, axis=0)
        row = lax.broadcasted_iota(jnp.int32, (SUM_ROW, rows), 0)
        inverse = 1.0 / jnp.where(row < GROUP, total, 1.0)
        column = lax.rem(s, wide) * width + lax.broadcasted_iota(
            jnp.int32, (2 * SUM_ROW, width), 1
        )
        pick = jnp.where(lax.div(column, HEAD) == index, 1.0, 0.0).astype(bf16)
        result = jnp.zeros((rows, width), f32)
        for i in range(lines):
            result = result + R.part_in[h][i].astype(f32) * spread(rescale[i] * inverse, pick)
        R.att[h][s] = result.astype(bf16)
        copy = pltpu.make_async_copy(R.att[h].at[s], R.attended.at[pl.ds(starts[h], rows)], R.o_sems.at[0])
        copy.start()


    def project(h, flow):
        total = R.own_tokens[part(h), :]
        for j in range(KV_HEADS):
            flow.take(j)
            g = at.group(j)
            block = jnp.concatenate([R.att[h][g * wide + i] for i in range(wide)], axis=1)
            total = total + times_transposed(block, R.w_out[g])
        R.residual[part(h), :] = total
        R.lined[h][hi] = (total * R.gain_ffn[...]).astype(bf16)
        R.squares[h][s] = column_to_row(jnp.sum(total * total, axis=1, keepdims=True))
        for d in range(1, lines):
            copy = push(
                R.lined[h].at[hi], R.lined[h].at[hi], sent[h].sem, R.l_sems.at[h, d - 1],
                (at.ahead(d) * 2 + lo, m),
            )
            sent[h].start(copy)
            lined[h].append(copy)
        relay(h, range(1))
        for d in range(1, n):
            copy = push(
                R.squares[h].at[s], R.squares[h].at[s], sent_squares[h].sem, R.sq_sems.at[h],
                (lax.rem(s + d, n), m),
            )
            sent_squares[h].start(copy)

    lined = [[] for _ in range(PARTS)]

    def relay(h, steps):
        for d in steps:
            if d:
                lined[h][d - 1].wait_recv()
            line = at.behind(d)
            source = line * 2 + lo
            to_m, k = source // per, lax.rem(source, per)
            for b in range(1 if FORWARD[h] else 2):
                copy = push(
                    R.lined[h].at[line], R.blocks[h].at[m, k], sent[h].sem, R.r_recv.at[h],
                    at.near(b, to_m),
                )
                if b:
                    sent[h].start(copy)
                    continue

                @pl.when(to_m == m)
                def _():
                    R.blocks[h][m, k] = R.lined[h][line]

                @pl.when(to_m != m)
                def _():
                    copy.start()

        if 0 in steps:
            sent[h].count += lines - per // 2

    order = (1 - core, 3 - core, core, 2 + core)

    def forward(h):
        if not FORWARD[h]:
            return
        arrival(R.sized[h], (n_mp - 1) * (per // 2), R.r_recv.at[h], at.partner).wait_recv()
        for k in range(per // 2):
            for t in range(n_mp):
                block = R.blocks[h].at[t, k * 2 + lo]
                copy = push(block, block, sent[h].sem, R.f_recv.at[h], at.partner)
                sent[h].start(copy)

    def collect(h):
        if FORWARD[h]:
            blocks = n_mp * (per // 2)
            arrival(R.sized[h], blocks, R.f_recv.at[h], at.partner).wait_recv()
        else:
            blocks = n_mp * per - per // 2
            arrival(R.sized[h], blocks, R.r_recv.at[h], at.partner).wait_recv()
        rows = sizes[h]
        for p, t in enumerate(order):
            R.features[h][p * rows : (p + 1) * rows, :] = jnp.concatenate(
                [R.blocks[h][t, j] for j in range(per)], axis=1
            )

    def inverse_of(h):
        arrival(R.sized_squares[h], n - 1, R.sq_sems.at[h], at.partner).wait_recv()
        return row_to_column(lax.rsqrt(jnp.sum(R.squares[h][...], axis=0) / D + eps))

    chunks = []
    for c, (h, first, last) in enumerate(bounds):
        kept, s1_out, s1_in, s2_out, s2_in, act = (
            getattr(R, f"{name}{c}") for name in ("kept", "s1_out", "s1_in", "s2_out", "s2_in", "act")
        )
        sem = lambda k, c=c: R.c_sems.at[c, k]
        chunks.append(
            dict(
                half=h, first=first, last=last, kept=kept, s1_out=s1_out, s1_in=s1_in,
                s2_out=s2_out, s2_in=s2_in, act=act,
                s1=push(s1_out, s1_in, sem(0), sem(1), at.sibling),
                s2=push(s2_out, s2_in, sem(0), sem(2), at.across),
                near=push(act.at[m], act.at[m], sem(0), sem(4), at.sibling),
                far=push(act.at[m], act.at[m], sem(0), sem(3), at.across),
                relay=push(
                    act.at[at.across[1]], act.at[at.across[1]], sem(0), sem(4), at.sibling
                ),
                both=arrival(getattr(R, f"chunk{c}"), 2, sem(4), at.sibling),
                sent=Sent(sem(0), getattr(R, f"chunk{c}"), at.partner),
            )
        )
    halves = [[ch for ch in chunks if ch["half"] == h] for h in range(PARTS)]

    def multiply(ch):
        for g, weight in enumerate((R.gate_w, R.up_w)):
            rows = sizes[ch["half"]]
            product = times_transposed(R.features[ch["half"]][...], weight[ch["first"] : ch["last"], :])
            for p in range(2):
                ch["s1_out"][g, p] = product[p * rows : (p + 1) * rows].astype(bf16)
                ch["kept"][g, p] = product[(p + 2) * rows : (p + 3) * rows]
        ch["s1"].start()

    def pair_sum(ch):
        ch["s1"].wait_recv()
        for g in range(2):
            ch["s2_out"][g] = (
                ch["kept"][g, 1 - y] + ch["s1_in"][g, 1 - y].astype(f32)
            ).astype(bf16)
        ch["s2"].start()

    def activate(ch, inverse):
        ch["s2"].wait_recv()
        gate, up = [
            (ch["kept"][g, y] + ch["s1_in"][g, y].astype(f32) + ch["s2_in"][g].astype(f32))
            * inverse
            for g in range(2)
        ]
        ch["act"][m] = (gate / (1.0 + jnp.exp(-gate)) * up).astype(bf16)
        ch["far"].start()
        ch["near"].start()

    def pass_on(ch):
        ch["far"].wait_recv()
        ch["relay"].start()

    def down(ch):
        h, own, rows = ch["half"], halves[ch["half"]], sizes[ch["half"]]
        ch["both"].wait_recv()
        act = ch["act"][...].reshape(n_mp * rows, ch["last"] - ch["first"])
        total = jnp.dot(act, R.down_w[ch["first"] : ch["last"], :], preferred_element_type=f32)
        if ch is not own[0]:
            total = R.acc[h][...] + total
        if ch is not own[-1]:
            R.acc[h][...] = total
            return
        for t in range(n_mp):
            for k in range(per):
                R.down_out[h][t, k % 2, k // 2] = total[
                    t * rows : (t + 1) * rows, k * width : (k + 1) * width
                ].astype(bf16)

    def leave(h):
        for i in range(n_mp):
            for b in range(2):
                if i == 0 and b == 0:
                    R.home_in[h][lo, m] = R.down_out[h][m, lo]
                    continue
                to_m, to_lo = lax.rem(m + i, n_mp), lax.rem(lo + b, 2)
                copy = push(
                    R.down_out[h].at[to_m, to_lo], R.home_in[h].at[lo, m], sent[h].sem,
                    R.h_sems.at[h, i], at.near(b, to_m),
                )
                sent[h].start(copy, per // 2)


    def send_home(h):
        for i in range(n_mp):
            source = lax.rem(m + n_mp - i, n_mp)
            blocks = (2 if i else 1) * (per // 2)
            arrival(R.sized[h], blocks, R.h_sems.at[h, i], at.partner).wait_recv()
            for k in range(per // 2):
                line = source * (per // 2) + k
                total = R.home_in[h][0, source, k].astype(f32) + R.home_in[h][1, source, k].astype(f32)
                R.home_out[h][line] = total.astype(bf16)
                copy = push(
                    R.home_out[h].at[line], R.terms[h].at[hi], sent[h].sem, R.t_recv.at[h],
                    (line * 2 + lo, m),
                )

                @pl.when(line == hi)
                def _():
                    R.terms[h][hi] = R.home_out[h][line]

                @pl.when(line != hi)
                def _():
                    copy.start()

        sent[h].count += lines - 1

    def conclude(h):
        arrival(R.sized[h], lines - 1, R.t_recv.at[h], at.partner).wait_recv()
        result = R.residual[part(h), :]
        for i in range(lines):
            result = result + R.terms[h][i].astype(f32)
        R.result[part(h), :] = result.astype(bf16)
        copy = pltpu.make_async_copy(
            R.result.at[pl.ds(starts[h], sizes[h])], R.out.at[pl.ds(starts[h], sizes[h])],
            R.o_sems.at[0],
        )
        copy.start()

    loads["keys"].wait()
    loads["values"].wait()
    waiting = []

    def score(h, j):
        asked[h].take(j)
        attend(h, j)
        waiting.append((h, j))
        if len(waiting) > LAG:
            join(*waiting.pop(0))

    answered = [Gather(at, R.att[h], R.a_sems.at[h], sent[h], ANSWER_STRAIGHT[h]) for h in range(PARTS)]

    def answer(h):
        merge(h)
        answered[h].start()

    score(0, 0)
    asked[0].hand_all()
    for h in range(PARTS):
        for j in range(KV_HEADS):
            if h or j:
                score(h, j)
            if h + 1 < PARTS and lines == KV_HEADS:
                asked[h + 1].hand(j)
        if h + 1 < PARTS:
            asked[h + 1].hand_all()
    for item in waiting[:-1]:
        join(*item)
    for g in range(KV_HEADS):
        loads[f"w_out{g}"].wait()
    loads["gain_ffn"].wait()
    answer(0)
    join(*waiting[-1])
    a, b = halves
    later = range(1, lines)
    answered[0].hand_all()
    answer(1)
    project(0, answered[0])
    answered[1].hand_all()
    relay(0, later)
    project(1, answered[1])
    loads["gate"].wait()
    loads["up"].wait()
    collect(0)
    multiply(a[0])
    relay(1, later)
    for before, ch in zip(a, a[1:]):
        multiply(ch)
        pair_sum(before)
    pair_sum(a[-1])
    inverse = [inverse_of(0)]
    loads["down"].wait()
    forward(1)
    activate(a[0], inverse[0])
    collect(1)
    multiply(b[0])
    inverse.append(inverse_of(1))
    for k, ch in enumerate(b[1:]):
        multiply(ch)
        pair_sum(b[k])
        if k + 1 < len(a):
            activate(a[k + 1], inverse[0])
    for ch in a[len(b) :]:
        activate(ch, inverse[0])
    pass_on(a[0])
    pair_sum(b[-1])
    for k, ch in enumerate(a):
        if k + 1 < len(a):
            pass_on(a[k + 1])
        down(ch)
        if k < len(b):
            activate(b[k], inverse[1])
    for ch in b[len(a) :]:
        activate(ch, inverse[1])
    leave(0)
    pass_on(b[0])
    for k, ch in enumerate(b):
        if k + 1 < len(b):
            pass_on(b[k + 1])
        down(ch)
    leave(1)
    for h in range(PARTS):
        send_home(h)
    for h in range(PARTS):
        conclude(h)

    pltpu.make_async_copy(R.sized_out, R.sized_out, R.o_sems.at[0]).wait()
    for record in sent + sent_stats + sent_squares:
        record.wait()
    for ch in chunks:
        ch["sent"].count = 9
        ch["sent"].wait()


def layer(n, n_mp, *arrays):
    tokens, w_query, keys, w_gate, w_down = (arrays[i] for i in (0, 2, 4, 8, 10))
    rows, width = tokens.shape[0], w_query.shape[0]
    hidden, quarter = w_gate.shape
    lines, per = n // 2, n // n_mp
    bounds = []
    for h in range(PARTS):
        cuts = [min(hidden, -(-int(hidden * cut) // 128) * 128) for cut in CUTS[h]] + [hidden]
        bounds += [(h, first, last) for first, last in zip([0] + cuts, cuts) if first < last]
    bf16, f32, dma = jnp.bfloat16, jnp.float32, pltpu.SemaphoreType.DMA
    scratch = dict(
        tokens=VMEM(tokens.shape, bf16),
        gain_attn=VMEM((D,), f32),
        bias=VMEM((1, width), f32),
        gain_ffn=VMEM((1, width), f32),
        w_query=VMEM((KV_HEADS, width, D // KV_HEADS), bf16),
        keys=VMEM(keys.shape, bf16),
        values=VMEM(keys.shape, bf16),
        w_out=VMEM((KV_HEADS, width, D // KV_HEADS), bf16),
        gate_w=VMEM(w_gate.shape, bf16),
        up_w=VMEM(w_gate.shape, bf16),
        down_w=VMEM(w_down.shape, bf16),
        sized_out=VMEM((2 * rows, width), bf16),
        own_tokens=VMEM((rows, width), f32),
        residual=VMEM((rows, width), f32),
        result=VMEM((rows, width), bf16),
        w_sems=dma((9 + 2 * KV_HEADS,)),
        s_sems=dma((3, PARTS)),
        q_sems=dma((PARTS, 2 * lines - 1)),
        a_sems=dma((PARTS, 2 * lines - 1)),
        p_sems=dma((PARTS, 2, KV_HEADS)),
        m_recv=dma((PARTS, 2)),
        o_sems=dma((1,)),
        l_sems=dma((PARTS, lines - 1)),
        sq_sems=dma((PARTS,)),
        r_recv=dma((PARTS,)),
        f_recv=dma((PARTS,)),
        h_sems=dma((PARTS, n_mp)),
        t_recv=dma((PARTS,)),
        c_sems=dma((len(bounds), 5)),
    )
    for h, part in enumerate(part_rows(rows)[1]):
        own = dict(
            qbuf=VMEM((n, part, width), bf16),
            part_out=VMEM((KV_HEADS, 2, n // KV_HEADS // 2, part, width), bf16),
            pair_in=VMEM((KV_HEADS, n // KV_HEADS // 2, part, width), bf16),
            line_out=VMEM((KV_HEADS, n // KV_HEADS // 2, part, width), bf16),
            part_in=VMEM((lines, part, width), bf16),
            stat_out=VMEM((KV_HEADS, 2 * SUM_ROW, part), f32),
            pair_stat=VMEM((KV_HEADS, 2 * SUM_ROW, part), f32),
            line_stat=VMEM((KV_HEADS, 2 * SUM_ROW, part), f32),
            stat_in=VMEM((lines, 2 * SUM_ROW, part), f32),
            att=VMEM((n, part, width), bf16),
            lined=VMEM((lines, part, width), bf16),
            squares=VMEM((n, 1, part), f32),
            blocks=VMEM((n_mp, per, part, width), bf16),
            features=VMEM((n_mp * part, quarter), bf16),
            acc=VMEM((n_mp * part, w_down.shape[1]), f32),
            down_out=VMEM((n_mp, 2, per // 2, part, width), bf16),
            home_in=VMEM((2, n_mp, per // 2, part, width), bf16),
            home_out=VMEM((lines, part, width), bf16),
            terms=VMEM((lines, part, width), bf16),
            sized=VMEM((8 * n, part, width), bf16),
            sized_stats=VMEM((2 * n, 2 * SUM_ROW, part), f32),
            sized_squares=VMEM((n, 1, part), f32),
        )
        scratch.update({f"{name}_{h}": ref for name, ref in own.items()})
    for c, (h, first, last) in enumerate(bounds):
        span, part = last - first, part_rows(rows)[1][h]
        buffers = dict(
            kept=VMEM((2, 2, part, span), f32),
            s1_out=VMEM((2, 2, part, span), bf16),
            s1_in=VMEM((2, 2, part, span), bf16),
            s2_out=VMEM((2, part, span), bf16),
            s2_in=VMEM((2, part, span), bf16),
            chunk=VMEM((9, part, span), bf16),
            act=VMEM((n_mp, part, span), bf16),
        )
        scratch.update({f"{name}{c}": ref for name, ref in buffers.items()})
    names = ARGS + OUTS + tuple(scratch)
    block = jax.ShapeDtypeStruct((rows, width), bf16)
    anywhere = pl.BlockSpec(memory_space=pl.ANY)
    return pl.pallas_call(
        functools.partial(layer_kernel, n, n_mp, bounds, tuple(own), names),
        out_shape=(block, block),
        in_specs=[anywhere] * len(ARGS),
        out_specs=(anywhere, anywhere),
        scratch_shapes=list(scratch.values()),
        compiler_params=pltpu.CompilerParams(
            collective_id=1, has_side_effects=True, vmem_limit_bytes=60 * 2**20
        ),
        name="layer",
    )(*arrays)


def results_kernel(attended, out, attended_out, layer_out, held, sems):
    pairs = ((attended, attended_out), (out, layer_out))
    into = [pltpu.make_async_copy(src, held.at[i], sems.at[0, i]) for i, (src, _) in enumerate(pairs)]
    back = [pltpu.make_async_copy(held.at[i], dst, sems.at[1, i]) for i, (_, dst) in enumerate(pairs)]
    for copy in into:
        copy.start()
    for copy, onward in zip(into, back):
        copy.wait()
        onward.start()
    for copy in back:
        copy.wait()


def results(attended, out):
    anywhere = pl.BlockSpec(memory_space=pl.ANY)
    block = jax.ShapeDtypeStruct(out.shape, out.dtype)
    return pl.pallas_call(
        results_kernel,
        out_shape=(block, block),
        in_specs=[anywhere, anywhere],
        out_specs=(anywhere, anywhere),
        scratch_shapes=[VMEM((2,) + out.shape, out.dtype), pltpu.SemaphoreType.DMA((2, 2))],
        name="results",
    )(attended, out)


def body(
    n_seq,
    n_mp,
    tokens,
    gain_attn,
    w_query,
    query_bias,
    cache_keys,
    cache_values,
    w_out,
    gain_ffn,
    w_gate,
    w_up,
    w_down,
):
    attended, out = layer(
        n_seq,
        n_mp,
        tokens,
        gain_attn,
        w_query.T,
        query_bias[None, :],
        cache_keys,
        cache_values,
        w_out.T,
        gain_ffn[None, :],
        w_gate.T,
        w_up.T,
        w_down,
    )
    return results(attended, out)


def solution(mesh):
    placed = (
        P("mp", None),
        P(),
        P(None, "seq"),
        P("seq"),
        P(None, "seq", None),
        P(None, "seq", None),
        P(None, "seq"),
        P("seq"),
        P("mp", "seq"),
        P("mp", "seq"),
        P("seq", "mp"),
    )
    return jax.shard_map(
        functools.partial(body, mesh.shape["seq"], mesh.shape["mp"]),
        mesh=mesh,
        in_specs=placed,
        out_specs=(P("mp", "seq"), P("mp", "seq")),
        check_vma=False,
    )
```
